32 devices in a mesh: row: 4 (over y, x), col: 4 (over z), depth: 2 (over core).
Axes of the slice: x: 2, y: 2, z: 4, core: 2. Of those that a mesh axis runs over, the one named last changes fastest.
Arguments:
- matrix_columns: float32 [4, 8, 768, 24576], P(None, ('col', 'depth'), None, 'row'), may hold values from -0.0390625 to 0.0390625
- sources: float32 [4, 8, 768, 128], P('row', ('col', 'depth')), may hold values from -6 to 6
Outputs:
- first_image: float32 [4, 8, 768, 128], P('row', ('col', 'depth'))
- second_image: float32 [4, 8, 768, 128], P('row', ('col', 'depth'))
The draws below stay inside these ranges and needn't reach their ends.
All inputs are finite; a program needn't handle non-finite values.
Results may differ from the reference program's by a relative error of at most 0.00011.
Values sent between devices are 32-bit elements; how exact they have to be, the bound alone decides.
A program may use at most 128 MiB of HBM per device.

```python
import jax
import jax.numpy as jnp
from jax import lax

ORDER = 24576
RHS = 128
PIECE = 768
N_ROW = 4
N_COL = 4
N_DEPTH = 2


def levels(key, shape, shards, least, high):
    gain = 1.0
    for position, parts in shards:
        draws = jax.random.uniform(jax.random.fold_in(jax.random.fold_in(key, 6), position), (parts,), jnp.float32, least / len(shards), high / len(shards))
        gain = gain * jnp.repeat(jnp.exp(draws), shape[position] // parts).reshape((-1,) + (1,) * (len(shape) - 1 - position))
    return gain


def noise(key, dims, width, limit, split=(), held_as=jnp.bfloat16):
    result = jax.random.normal(key, dims, jnp.float32) * width
    if len(split) > 0:
        result = levels(key, dims, split, -0.22, 0.18) * result
    return jnp.clip(result, min=-limit, max=limit).astype(held_as)


def setup_inputs(seed: int = 0) -> dict:
    keys = jax.random.split(jax.random.key(seed), 3)
    matrix_columns = noise(keys[0], (N_ROW, N_COL * N_DEPTH, PIECE, ORDER), ORDER ** -0.5, 0.0390625, ((1, 8), (3, 4)), jnp.float32)
    sources = noise(keys[1], (N_ROW, N_COL * N_DEPTH, PIECE, RHS), 1.0, 6.0, ((0, 4), (1, 8)), jnp.float32)
    return {"matrix_columns": matrix_columns, "sources": sources}


def apply_matrix(matrix_t, vectors):
    return lax.dot_general(matrix_t, vectors, (((0,), (0,)), ((), ())), precision=lax.Precision.HIGHEST, preferred_element_type=jnp.float32)


def reference(matrix_columns, sources):
    matrix_t = matrix_columns.reshape(ORDER, ORDER)
    inputs_flat = sources.reshape(ORDER, RHS)
    first_flat = apply_matrix(matrix_t, inputs_flat)
    second_flat = apply_matrix(matrix_t, first_flat)
    return first_flat.reshape(sources.shape), second_flat.reshape(sources.shape)
```

```python
import functools

import jax
import jax.numpy as jnp
from jax import lax
from jax.experimental import pallas as pl
from jax.experimental.pallas import tpu as pltpu
from jax.sharding import PartitionSpec as P

LANES = 256


def split(values):
    high = values.astype(jnp.bfloat16)
    low = (values - high.astype(jnp.float32)).astype(jnp.bfloat16)
    return high, low


def product_kernel(x_ref, a_ref, out_ref, xt_ref):
    width = x_ref.shape[1]
    depth = x_ref.shape[0]
    tile = a_ref.shape[3]

    @pl.when(pl.program_id(0) == 0)
    def _():
        high, low = split(x_ref[...].T)
        xt_ref[:width, :] = high
        xt_ref[width:, :] = low

    for start in range(0, tile, LANES):
        block = a_ref[:, 0, :, start:start + LANES].reshape(depth, LANES)
        high, low = split(block)
        main = jnp.dot(xt_ref[...], high, preferred_element_type=jnp.float32)
        rest = jnp.dot(xt_ref[:width, :], low, preferred_element_type=jnp.float32)
        total = main[:width] + (main[width:] + rest)
        out_ref[start:start + LANES, :] = total.T


def product(columns, inputs_flat):
    outer, _, piece, rows = columns.shape
    depth, width = inputs_flat.shape
    tile = 2 * LANES
    return pl.pallas_call(
        product_kernel,
        grid=(rows // tile,),
        out_shape=jax.ShapeDtypeStruct((rows, width), jnp.float32),
        in_specs=[
            pl.BlockSpec((depth, width), lambda i: (0, 0)),
            pl.BlockSpec((outer, 1, piece, tile), lambda i: (0, 0, 0, i)),
        ],
        out_specs=pl.BlockSpec((tile, width), lambda i: (i, 0)),
        scratch_shapes=[pltpu.VMEM((2 * width, depth), jnp.bfloat16)],
        compiler_params=pltpu.CompilerParams(
            dimension_semantics=("arbitrary",), vmem_limit_bytes=48 << 20
        ),
        cost_estimate=pl.CostEstimate(
            flops=6 * rows * depth * width, bytes_accessed=4 * rows * depth, transcendentals=0
        ),
    )(inputs_flat, columns)


def apply_once(columns, vector_part):
    piece_len = vector_part.shape[2]
    width = vector_part.shape[3]
    gathered = lax.all_gather(vector_part, "row", axis=0, tiled=True)
    inputs_flat = gathered.reshape(-1, width)
    owned = lax.psum_scatter(
        product(columns, inputs_flat), ("col", "depth"), scatter_dimension=0, tiled=True
    )
    return owned.reshape(1, 1, piece_len, width)


def body(matrix_columns, sources):
    first_image = apply_once(matrix_columns, sources)
    second_image = apply_once(matrix_columns, first_image)
    return (first_image, second_image)


def solution(mesh):
    in_specs = (P(None, ("col", "depth"), None, "row"), P("row", ("col", "depth"), None, None))
    out_specs = (P("row", ("col", "depth"), None, None), P("row", ("col", "depth"), None, None))
    return jax.shard_map(body, mesh=mesh, in_specs=in_specs, out_specs=out_specs, check_vma=False)
```
